32 devices in a mesh: expert: 4 (over y, core), mp: 8 (over z, x).
Axes of the slice: x: 2, y: 2, z: 4, core: 2. Of those that a mesh axis runs over, the one named last changes fastest.
Arguments:
- tokens: bfloat16 [512, 6144], P(('expert', 'mp')), may hold values from -18 to 18
- norm_gain: bfloat16 [6144], replicated, may hold values from 0.099609375 to 1.8984375
- expert_ids: int32 [512, 2], P(('expert', 'mp')), may hold values from 0 to 3, as said below
- slot_ids: int32 [512, 2], P(('expert', 'mp')), may hold values from 0 to 7, as said below
- route_weights: float32 [512, 2], P(('expert', 'mp')), may hold values from 0.1 to 1
- w_gate: bfloat16 [4, 6144, 8192], P('expert', None, 'mp'), may hold values from -0.078125 to 0.078125
- w_up: bfloat16 [4, 6144, 8192], P('expert', None, 'mp'), may hold values from -0.078125 to 0.078125
- w_down: bfloat16 [4, 8192, 6144], P('expert', 'mp'), may hold values from -0.0625 to 0.0625
Outputs:
- moe_out: bfloat16 [512, 6144], P(('expert', 'mp'))
The draws below stay inside these ranges and needn't reach their ends.
Inputs may be any that keep to these rules, and one draw needn't show every extreme that they name: `expert_ids`: each token names two different experts. Among the 16 tokens of one device (aligned blocks of rows) no expert is named more than 8 times, and on every device some expert is named exactly 8 times. `slot_ids`: within the tokens of one device, the entries that name the same expert have different slots; slots that no entry names stay empty.
All inputs are finite; a program needn't handle non-finite values.
Results may differ from the reference program's by a relative error of at most 0.015.
Values may be sent and summed in bfloat16 or wider, within the bound.
No kernel may reach another device: no remote copies, remote signals or barrier semaphores. Data moves between devices by JAX's collectives and lax.ppermute only.
A program may use at most 128 MiB of HBM per device.

```python
import math
import jax
import jax.numpy as jnp
from jax import lax

D = 6144
FF = 8192
EXPERTS = 4
TOK_DEV = 16
CAP = 8
TOKENS = 512
N_MP = 8


def route_tables(key):
    blocks = TOKENS // TOK_DEV

    def one_block(index):
        block_key = jax.random.fold_in(key, index)
        key_busy, key_pool, key_slot, key_order = jax.random.split(block_key, 4)
        busiest = jax.random.randint(key_busy, (), 0, EXPERTS)
        labels = jnp.arange((EXPERTS - 1) * CAP, dtype=jnp.int32) // CAP
        others = labels + (labels >= busiest).astype(jnp.int32)
        mixing = jax.random.permutation(key_pool, (EXPERTS - 1) * CAP)
        chosen = others[mixing[:2 * TOK_DEV - CAP]]
        sequence = jnp.sort(jnp.concatenate([jnp.full((CAP,), busiest, jnp.int32), chosen]))
        below = jnp.sum((sequence[None, :] < sequence[:, None]).astype(jnp.int32), axis=1)
        within = jnp.arange(2 * TOK_DEV, dtype=jnp.int32) - below
        tables = jax.vmap(lambda expert: jax.random.permutation(jax.random.fold_in(key_slot, expert), CAP))(jnp.arange(EXPERTS))
        slot_sequence = tables[sequence, within].astype(jnp.int32)
        token_order = jax.random.permutation(key_order, TOK_DEV)
        chosen_ids = jnp.stack([sequence[token_order], sequence[TOK_DEV + token_order]], axis=1)
        chosen_slots = jnp.stack([slot_sequence[token_order], slot_sequence[TOK_DEV + token_order]], axis=1)
        return (chosen_ids, chosen_slots)
    all_ids, all_slots = jax.vmap(one_block)(jnp.arange(blocks))
    return (all_ids.reshape(TOKENS, 2).astype(jnp.int32), all_slots.reshape(TOKENS, 2).astype(jnp.int32))


def draw_expert_ids(key, part):
    return route_tables(jax.random.fold_in(key, 7))[0]


def draw_slot_ids(key, part):
    return route_tables(jax.random.fold_in(key, 7))[1]


def draw_tokens(key, part):
    key_base, key_scale = jax.random.split(jax.random.fold_in(key, 3))
    base = jnp.clip(jax.random.normal(key_base, (TOKENS, D), jnp.float32), -6.0, 6.0)
    scale = jnp.exp(jax.random.uniform(key_scale, (TOKENS, 1), jnp.float32, math.log(0.3), math.log(3.0)))
    return (base * scale).astype(jnp.bfloat16)


def steps_of(own_key, dims, shards, least, largest):
    factor_of, own = 1.0, jax.random.fold_in(own_key, 6)
    for axis_at, parts in shards:
        steps = jnp.exp(jax.random.uniform(jax.random.fold_in(own, axis_at), (parts,), jnp.float32, least / len(shards), largest / len(shards)))
        factor_of = factor_of * jnp.repeat(steps, dims[axis_at] // parts).reshape([-1 if axis == axis_at else 1 for axis in range(len(dims))])
    return factor_of


def normal_values(rng, extent, scale, bound, shards=(), held_as=jnp.bfloat16):
    gain = steps_of(rng, extent, shards, -0.22, 0.18) if shards else 1.0
    entries = jax.random.normal(rng, extent, jnp.float32) * scale * gain
    return jnp.minimum(jnp.maximum(entries, -bound), bound).astype(held_as)


def setup_inputs(seed: int = 0) -> dict:
    key_of = jax.random.split(jax.random.key(seed), 9)
    return {
        "tokens": draw_tokens(jax.random.fold_in(key_of[8], 71), 0),
        "norm_gain": jnp.clip(1.0 + 0.18 * jax.random.normal(key_of[1], (D,), jnp.float32), 0.099609375, 1.8984375).astype(jnp.bfloat16),
        "expert_ids": draw_expert_ids(jax.random.fold_in(key_of[8], 71), 0),
        "slot_ids": draw_slot_ids(jax.random.fold_in(key_of[8], 71), 0),
        "route_weights": jnp.clip(jnp.exp(math.log(1.0) - 2.3025851 * jax.random.uniform(key_of[4], (TOKENS, 2), jnp.float32) ** steps_of(key_of[4], (TOKENS, 2), ((0, 32),), -0.2, 0.2)), 0.1, 1.0),
        "w_gate": normal_values(key_of[5], (EXPERTS, D, FF), D ** -0.5, 0.078125, ((0, 4), (2, 8))),
        "w_up": normal_values(key_of[6], (EXPERTS, D, FF), D ** -0.5, 0.078125, ((0, 4), (2, 8))),
        "w_down": normal_values(key_of[7], (EXPERTS, FF, D), FF ** -0.5, 0.0625, ((0, 4), (1, 8))),
    }


def reference(tokens, norm_gain, expert_ids, slot_ids, route_weights, w_gate, w_up, w_down):
    values = tokens.astype(jnp.float32)
    mean_square = lax.optimization_barrier(jnp.mean(values * values, axis=1, keepdims=True))
    normed = (values * lax.rsqrt(mean_square + 1e-05) * norm_gain.astype(jnp.float32)).astype(jnp.bfloat16)
    block_index = (jnp.arange(TOKENS, dtype=jnp.int32) // TOK_DEV).astype(jnp.int32)
    row_index = (block_index[:, None] * CAP + slot_ids).astype(jnp.int32)
    expert_rows = TOKENS // TOK_DEV * CAP
    buffer = jnp.zeros((EXPERTS, expert_rows, D), jnp.bfloat16)
    filled = jnp.broadcast_to(normed[:, None, :], (TOKENS, 2, D))
    buffer = buffer.at[expert_ids, row_index].set(filled)
    share_width = FF // N_MP

    def one_expert(operands):
        block, gate_mat, up_mat, down_mat = operands
        gate_proj = jnp.dot(block, gate_mat, preferred_element_type=jnp.float32)
        up_proj = jnp.dot(block, up_mat, preferred_element_type=jnp.float32)
        hidden = (jax.nn.silu(gate_proj) * up_proj).astype(jnp.bfloat16)

        def add_share(total, index):
            first = (index * share_width).astype(jnp.int32)
            part_hidden = lax.dynamic_slice_in_dim(hidden, first, share_width, 1)
            part_down = lax.dynamic_slice_in_dim(down_mat, first, share_width, 0)
            product = jnp.dot(part_hidden, part_down, preferred_element_type=jnp.float32).astype(jnp.bfloat16)
            product = lax.optimization_barrier(product)
            return (total + product.astype(jnp.float32), None)
        start_total = jnp.zeros((expert_rows, D), jnp.float32)
        total, unused = lax.scan(add_share, start_total, jnp.arange(N_MP, dtype=jnp.int32))
        return total.astype(jnp.bfloat16)
    expert_out = lax.map(one_expert, (buffer, w_gate, w_up, w_down))
    shares = route_weights / (route_weights[:, 0:1] + route_weights[:, 1:2])
    picked = expert_out[expert_ids, row_index].astype(jnp.float32)
    mixed = lax.optimization_barrier(jnp.sum(shares[:, :, None] * picked, axis=1))
    return mixed.astype(jnp.bfloat16)
```

```python
import jax
import jax.numpy as jnp
from jax import lax
from jax.sharding import PartitionSpec as P

CAP = 8
META = 128
AXES = ("expert", "mp")


class Grid:
    def __init__(self, sizes):
        self.cores = 2
        self.y = sizes["expert"] // self.cores
        self.x = self.y if sizes["mp"] % self.y == 0 else 1
        self.z = sizes["mp"] // self.x

    def index(self, y, c, z, x):
        return ((y * self.cores + c) * self.z + z) * self.x + x

    def move(self, value, to):
        pairs = []
        for y in range(self.y):
            for c in range(self.cores):
                for z in range(self.z):
                    for x in range(self.x):
                        target = to(y, c, z, x)
                        if target is not None:
                            pairs.append((self.index(y, c, z, x), self.index(*target)))
        return lax.ppermute(value, AXES, pairs)

    def first(self, k):
        return lambda y, c, z, x: (
            (y, c, z, (x + k) % self.x) if c == 0 else ((y + k) % self.y, c, z, x)
        )

    def second(self, k):
        return lambda y, c, z, x: (
            ((y + k) % self.y, c, z, x) if c == 0 else (y, c, z, (x + k) % self.x)
        )

    def sibling(self, y, c, z, x):
        return (y, 1 - c, z, x)

    def along_z(self, k):
        return lambda y, c, z, x: (y, c, (z + k) % self.z, x)


def z_pair(y, c, z, x):
    return (y, c, z ^ 1, x)


def z_middle(y, c, z, x):
    return (y, c, 3 - z, x) if z in (1, 2) else None


def z_out(y, c, z, x):
    return (y, c, {1: 0, 2: 3}[z], x) if z in (1, 2) else None


def z_in(y, c, z, x):
    return (y, c, {0: 1, 3: 2}[z], x) if z in (0, 3) else None


def gather_z(grid, own, inner):
    if grid.z != 4:
        return [own] + [grid.move(own, grid.along_z(k)) for k in range(1, grid.z)]
    near = grid.move(own, z_pair)
    across = grid.move(own, z_middle)
    far = grid.move(near, z_middle)
    passed = grid.move(across, z_out)
    last = grid.move(far, z_out)
    return [own, near, jnp.where(inner, across, passed), jnp.where(inner, far, last)]


def scatter_z(grid, parts, inner):
    if grid.z != 4:
        total = parts[0]
        for k in range(1, grid.z):
            total = total + grid.move(parts[k], grid.along_z(-k))
        return total
    own, near, second, third = parts
    third = third + grid.move(third, z_in)
    near = near + grid.move(third, z_middle)
    second = second + grid.move(second, z_in)
    return own + grid.move(second, z_middle) + grid.move(near, z_pair)


def spread(grid, block):
    firsts = [block] + [grid.move(block, grid.first(k)) for k in range(1, grid.x)]
    half = jnp.concatenate(firsts, axis=0)
    seconds = [half] + [grid.move(half, grid.second(k)) for k in range(1, grid.y)]
    return jnp.concatenate(seconds, axis=0)


def fold(grid, rows):
    size = rows.shape[0] // grid.y
    half = rows[:size]
    for k in range(1, grid.y):
        half = half + grid.move(rows[k * size : (k + 1) * size], grid.second(-k))
    size = size // grid.x
    block = half[:size]
    for k in range(1, grid.x):
        block = block + grid.move(half[k * size : (k + 1) * size], grid.first(-k))
    return block


def local(grid, tokens, norm_gain, expert_ids, slot_ids, route_weights, w_gate, w_up, w_down):
    features = tokens.shape[1]
    f32, bf16 = jnp.float32, jnp.bfloat16
    values = tokens.astype(f32)
    mean_square = jnp.mean(values * values, axis=1, keepdims=True)
    normed = (values * lax.rsqrt(mean_square + 1e-05) * norm_gain.astype(f32)).astype(bf16)
    shares = route_weights / (route_weights[:, 0:1] + route_weights[:, 1:2])
    high = lax.reduce_precision(shares, 8, 7)
    middle = lax.reduce_precision(shares - high, 8, 7)
    low = shares - high - middle
    target = (expert_ids * CAP + slot_ids).astype(f32)
    meta = jnp.concatenate([target, high, middle, low], axis=1).astype(bf16)
    meta = jnp.pad(meta, ((0, 0), (0, META - meta.shape[1])))
    own = jnp.concatenate([normed, meta], axis=1)

    expert = lax.axis_index("expert")
    z = lax.axis_index("mp") // grid.x
    inner = (z == 1) | (z == 2)
    groups = [spread(grid, block) for block in gather_z(grid, own, inner)]
    theirs = [grid.move(group, grid.sibling) for group in groups]
    known = jnp.concatenate(groups + theirs, axis=0)

    count = known.shape[0]
    tok_rows = tokens.shape[0]
    rows = count // tok_rows * CAP
    meta = known[:, features : features + 8].astype(f32)
    slots = meta[:, 0:2] - (expert * CAP).astype(f32)
    here = (slots >= 0) & (slots < CAP)
    block = (lax.broadcasted_iota(jnp.int32, (count, 2), 0) // tok_rows * CAP).astype(f32)
    places = jnp.where(here, slots + block, -1.0)
    index = lax.broadcasted_iota(jnp.int32, (rows, count), 0).astype(f32)
    hit = [index == places[None, :, k] for k in range(2)]
    placing = (hit[0] | hit[1]).astype(bf16)
    share = meta[:, 2:4] + meta[:, 4:6] + meta[:, 6:8]
    weight = sum(jnp.sum(jnp.where(hit[k], share[None, :, k], 0.0), axis=1) for k in range(2))
    piece = jnp.dot(placing, known[:, :features], preferred_element_type=f32).astype(bf16)
    gate_proj = jnp.dot(piece, w_gate[0], preferred_element_type=f32)
    up_proj = jnp.dot(piece, w_up[0], preferred_element_type=f32)
    hidden = (jax.nn.silu(gate_proj) * up_proj * weight[:, None]).astype(bf16)
    product = jnp.dot(hidden, w_down[0], preferred_element_type=f32).astype(bf16)
    spreading = placing.T
    half = count // 2
    away = jnp.dot(spreading[half:], product, preferred_element_type=f32).astype(bf16)
    kept = jnp.dot(spreading[:half], product, preferred_element_type=f32).astype(bf16)

    size = half // grid.z
    parts = []
    for k in reversed(range(grid.z)):
        place = slice(k * size, (k + 1) * size)
        parts.append(fold(grid, kept[place] + grid.move(away[place], grid.sibling)))
    return scatter_z(grid, parts[::-1], inner)


def solution(mesh):
    grid = Grid(mesh.shape)
    placed = (
        P(("expert", "mp"), None),
        P(),
        P(("expert", "mp"), None),
        P(("expert", "mp"), None),
        P(("expert", "mp"), None),
        P("expert", None, "mp"),
        P("expert", None, "mp"),
        P("expert", "mp", None),
    )

    def body(*args):
        return local(grid, *args)

    return jax.shard_map(
        body, mesh=mesh, in_specs=placed, out_specs=P(("expert", "mp"), None), check_vma=False
    )
```

```python
import functools

import jax
import jax.numpy as jnp
from jax import lax
from jax.experimental import pallas as pl
from jax.experimental.pallas import tpu as pltpu
from jax.sharding import PartitionSpec as P


CAP = 8
META = 128
FFT = 256
OUT = 1024
PLACE = 2048
MIX = 2048
FFN_VMEM = 32 * 2**20
AXES = ("expert", "mp")


class Grid:
    def __init__(self, sizes):
        self.cores = 2
        self.y = sizes["expert"] // self.cores
        self.x = self.y if sizes["mp"] % self.y == 0 else 1
        self.z = sizes["mp"] // self.x

    def index(self, y, c, z, x):
        return ((y * self.cores + c) * self.z + z) * self.x + x

    def move(self, value, to):
        pairs = []
        for y in range(self.y):
            for c in range(self.cores):
                for z in range(self.z):
                    for x in range(self.x):
                        target = to(y, c, z, x)
                        if target is not None:
                            pairs.append((self.index(y, c, z, x), self.index(*target)))
        return lax.ppermute(value, AXES, pairs)

    def first(self, k):
        return lambda y, c, z, x: (
            (y, c, z, (x + k) % self.x) if c == 0 else ((y + k) % self.y, c, z, x)
        )

    def second(self, k):
        return lambda y, c, z, x: (
            ((y + k) % self.y, c, z, x) if c == 0 else (y, c, z, (x + k) % self.x)
        )

    def sibling(self, y, c, z, x):
        return (y, 1 - c, z, x)

    def across_z(self, k, sign=1):
        if self.z & (self.z - 1) == 0:
            return lambda y, c, z, x: (y, c, z ^ k, x)
        return lambda y, c, z, x: (y, c, (z + sign * k) % self.z, x)


def gather_z(grid, own):
    blocks = [own] + [None] * (grid.z - 1)
    for k in reversed(range(1, grid.z)):
        blocks[k] = grid.move(own, grid.across_z(k))
    return blocks


def scatter_z(grid, parts):
    total = parts[0].astype(jnp.float32)
    for k in range(1, grid.z):
        moved = grid.move(parts[k], grid.across_z(k, -1))
        total = total + moved.astype(jnp.float32)
    return total.astype(jnp.bfloat16)


def spread(grid, block):
    firsts = [block] + [grid.move(block, grid.first(k)) for k in range(1, grid.x)]
    half = jnp.concatenate(firsts, axis=0)
    seconds = [half] + [grid.move(half, grid.second(k)) for k in range(1, grid.y)]
    return jnp.concatenate(seconds, axis=0)


def fold(grid, rows):
    size = rows.shape[0] // grid.y
    moved = [grid.move(rows[k * size : (k + 1) * size], grid.second(-k)) for k in range(1, grid.y)]
    half = sum(moved, rows[:size])
    size = size // grid.x
    moved = [grid.move(half[k * size : (k + 1) * size], grid.first(-k)) for k in range(1, grid.x)]
    return sum(moved, half[:size])


def prepare_kernel(tok_ref, gain_ref, ids_ref, slots_ref, route_ref, out_ref):
    f32, bf16 = jnp.float32, jnp.bfloat16
    _, features = tok_ref.shape
    values = tok_ref[...].astype(f32)
    mean_square = jnp.mean(values * values, axis=1, keepdims=True)
    scale = lax.rsqrt(mean_square + 1e-05)
    for at in range(gain_ref.shape[0]):
        place = slice(at * 128, (at + 1) * 128)
        gain = gain_ref[at : at + 1, :].astype(f32)
        out_ref[:, place] = (values[:, place] * scale * gain).astype(bf16)
    target = (ids_ref[...] * CAP + slots_ref[...]).astype(f32)
    route = route_ref[...]
    shares = route / (route[0:1] + route[1:2])
    high = shares.astype(bf16).astype(f32)
    middle = (shares - high).astype(bf16).astype(f32)
    low = shares - high - middle
    parts = jnp.concatenate([target, high, middle, low], axis=0).astype(bf16)
    row = lax.broadcasted_iota(jnp.int32, (parts.shape[0], META), 0)
    lane = lax.broadcasted_iota(jnp.int32, (parts.shape[0], META), 1)
    select = (row == lane).astype(bf16)
    turned = lax.dot_general(
        parts, select, (((0,), (0,)), ((), ())), preferred_element_type=f32
    )
    out_ref[:, features:] = turned.astype(bf16)


def prepare(tokens, norm_gain, expert_ids, slot_ids, route_weights):
    rows, features = tokens.shape
    return pl.pallas_call(
        prepare_kernel,
        out_shape=jax.ShapeDtypeStruct((rows, features + META), jnp.bfloat16),
        name="prepare",
    )(tokens, norm_gain.reshape(-1, 128), expert_ids.T, slot_ids.T, route_weights.T)


def hits(metas, expert, tok_rows, cores):
    meta = jnp.concatenate(metas, axis=0).astype(jnp.float32)
    count = meta.shape[0]
    each = count // tok_rows * CAP
    block = lax.broadcasted_iota(jnp.int32, (count, 2), 0) // tok_rows * CAP
    places = jnp.full((count, 2), -1.0, jnp.float32)
    for side in range(cores):
        first = ((expert ^ side) * CAP).astype(jnp.float32)
        slots = meta[:, 0:2] - first
        here = (slots >= 0) & (slots < CAP)
        places = jnp.where(here, slots + (block + side * each).astype(jnp.float32), places)
    index = lax.broadcasted_iota(jnp.int32, (count, cores * each), 1).astype(jnp.float32)
    share = meta[:, 2:4] + meta[:, 4:6] + meta[:, 6:8]
    return [index == places[:, k : k + 1] for k in range(2)], share


def place_kernel(n, tok_rows, features, *refs):
    f32, bf16 = jnp.float32, jnp.bfloat16
    blocks, outs = refs[:n], refs[n:]
    expert = lax.axis_index("expert")
    hit, _ = hits([b[:, features:] for b in blocks], expert, tok_rows, len(outs))
    placing = (hit[0] | hit[1]).astype(f32).T.astype(bf16)
    each = outs[0].shape[0]

    @pl.loop(0, features // PLACE)
    def _(j):
        place = pl.ds(pl.multiple_of(j * PLACE, PLACE), PLACE)
        known = jnp.concatenate([b[:, place] for b in blocks], axis=0)
        got = jnp.dot(placing, known, preferred_element_type=f32).astype(bf16)
        for side, out in enumerate(outs):
            out[:, place] = got[side * each : (side + 1) * each]


def place_rows(groups, tok_rows, features):
    count = sum(g.shape[0] for g in groups)
    each = count // tok_rows * CAP
    vmem = pl.BlockSpec(memory_space=pltpu.VMEM)
    out = jax.ShapeDtypeStruct((each, features), jnp.bfloat16)
    return pl.pallas_call(
        functools.partial(place_kernel, len(groups), tok_rows, features),
        out_shape=[out] * 2,
        in_specs=[vmem] * len(groups),
        out_specs=[vmem] * 2,
        cost_estimate=pl.CostEstimate(
            flops=4 * count * each * features, bytes_accessed=4 * count * features, transcendentals=0
        ),
        compiler_params=pltpu.CompilerParams(vmem_limit_bytes=count * 28 * 2**10),
        name="place",
    )(*groups)


def ffn_kernel(features, mine, theirs, gate, up_hbm, down_hbm, out_mine, out_theirs, *scratch):
    f32, bf16 = jnp.float32, jnp.bfloat16
    up, down, gated, hidden, up_sems, down_sems = scratch
    width, each = gate.shape[2], mine.shape[0]
    up_tiles, down_tiles = width // FFT, features // OUT

    def piece():
        return jnp.concatenate([mine[...], theirs[...]], axis=0)

    def tile(i, size):
        return pl.ds(pl.multiple_of(i * size, size), size)

    def up_copy(i):
        place = tile(i, FFT)
        return pltpu.make_async_copy(up_hbm.at[0, :, place], up.at[:, place], up_sems.at[i])

    def down_copy(i):
        place = tile(i, OUT)
        return pltpu.make_async_copy(down_hbm.at[0, :, place], down.at[:, place], down_sems.at[i])

    for i in range(up_tiles):
        up_copy(i).start()

    @pl.loop(0, up_tiles)
    def _(i):
        gate_proj = jnp.dot(piece(), gate[0, :, tile(i, FFT)], preferred_element_type=f32)
        gated[:, tile(i, FFT)] = gate_proj / (1.0 + jnp.exp(-gate_proj))

    for i in range(down_tiles):
        down_copy(i).start()

    @pl.loop(0, up_tiles)
    def _(i):
        up_copy(i).wait()
        up_proj = jnp.dot(piece(), up[:, tile(i, FFT)], preferred_element_type=f32)
        hidden[:, tile(i, FFT)] = (gated[:, tile(i, FFT)] * up_proj).astype(bf16)

    @pl.loop(0, down_tiles)
    def _(i):
        down_copy(i).wait()
        place = tile(i, OUT)
        product = jnp.dot(hidden[...], down[:, place], preferred_element_type=f32)
        product = product.astype(bf16)
        out_mine[:, place] = product[:each]
        out_theirs[:, place] = product[each:]


def ffn(mine, theirs, w_gate, w_up, w_down):
    bf16 = jnp.bfloat16
    each, features = mine.shape
    width = w_gate.shape[2]
    need = 2 * (3 * features * width + 4 * each * features + 2 * each * width)
    if need > 56 * 2**20 or width % FFT or features % OUT:
        piece = jnp.concatenate([mine, theirs], axis=0)
        gate_proj = jnp.dot(piece, w_gate[0], preferred_element_type=jnp.float32)
        up_proj = jnp.dot(piece, w_up[0], preferred_element_type=jnp.float32)
        hidden = (jax.nn.silu(gate_proj) * up_proj).astype(bf16)
        product = jnp.dot(hidden, w_down[0], preferred_element_type=jnp.float32).astype(bf16)
        return product[:each], product[each:]
    vmem, hbm = pl.BlockSpec(memory_space=pltpu.VMEM), pl.BlockSpec(memory_space=pltpu.HBM)
    return pl.pallas_call(
        functools.partial(ffn_kernel, features),
        out_shape=[jax.ShapeDtypeStruct(mine.shape, bf16)] * 2,
        in_specs=[vmem] * 3 + [hbm] * 2,
        out_specs=[vmem] * 2,
        scratch_shapes=[
            pltpu.VMEM((features, width), bf16),
            pltpu.VMEM((width, features), bf16),
            pltpu.VMEM((2 * each, width), jnp.float32),
            pltpu.VMEM((2 * each, width), bf16),
            pltpu.SemaphoreType.DMA((width // FFT,)),
            pltpu.SemaphoreType.DMA((features // OUT,)),
        ],
        cost_estimate=pl.CostEstimate(
            flops=12 * each * features * width,
            bytes_accessed=6 * features * width,
            transcendentals=2 * each * width,
        ),
        compiler_params=pltpu.CompilerParams(vmem_limit_bytes=FFN_VMEM),
        name="ffn",
    )(mine, theirs, w_gate, w_up, w_down)


def mix_kernel(n, tok_rows, features, *refs):
    f32, bf16 = jnp.float32, jnp.bfloat16
    metas, (mine, theirs), outs = refs[:n], refs[n : n + 2], refs[n + 2 :]
    expert = lax.axis_index("expert")
    hit, share = hits([m[...] for m in metas], expert, tok_rows, 2)
    taking = [h.astype(f32).astype(bf16) for h in hit]

    @pl.loop(0, features // MIX)
    def _(j):
        place = pl.ds(pl.multiple_of(j * MIX, MIX), MIX)
        product = jnp.concatenate([mine[:, place], theirs[:, place]], axis=0)
        total = share[:, 0:1] * jnp.dot(taking[0], product, preferred_element_type=f32)
        total += share[:, 1:2] * jnp.dot(taking[1], product, preferred_element_type=f32)
        total = total.astype(bf16)
        at = 0
        for out in outs:
            out[:, place] = total[at : at + out.shape[0]]
            at += out.shape[0]


def mix(groups, mine, theirs, tok_rows):
    features = mine.shape[1]
    n = len(groups)
    vmem = pl.BlockSpec(memory_space=pltpu.VMEM)
    last = features // META
    metas = [
        pl.BlockSpec((g.shape[0], META), lambda i: (0, last), memory_space=pltpu.VMEM) for g in groups
    ]
    whole = pl.BlockSpec(mine.shape, lambda i: (0, 0))
    count = sum(g.shape[0] for g in groups)
    return pl.pallas_call(
        functools.partial(mix_kernel, n, tok_rows, features),
        grid=(1,),
        out_shape=[jax.ShapeDtypeStruct((g.shape[0], features), jnp.bfloat16) for g in groups],
        in_specs=metas + [whole] * 2,
        out_specs=[pl.BlockSpec((g.shape[0], features), lambda i: (0, 0)) for g in groups],
        cost_estimate=pl.CostEstimate(
            flops=8 * count * mine.shape[0] * features,
            bytes_accessed=4 * count * features,
            transcendentals=0,
        ),
        compiler_params=pltpu.CompilerParams(vmem_limit_bytes=count * 28 * 2**10),
        name="mix",
    )(*groups, mine, theirs)


def local(grid, tokens, norm_gain, expert_ids, slot_ids, route_weights, w_gate, w_up, w_down):
    tok_rows, features = tokens.shape
    own = prepare(tokens, norm_gain, expert_ids, slot_ids, route_weights)
    groups = [spread(grid, block) for block in gather_z(grid, own)]
    mine, away = place_rows(groups, tok_rows, features)
    theirs = grid.move(away, grid.sibling)
    mine, away = ffn(mine, theirs, w_gate, w_up, w_down)
    theirs = grid.move(away, grid.sibling)
    parts = list(mix(groups, mine, theirs, tok_rows))
    for k in reversed(range(grid.z)):
        parts[k] = fold(grid, parts[k])
    return scatter_z(grid, parts)


def solution(mesh):
    grid = Grid(mesh.shape)
    placed = (
        P(("expert", "mp"), None),
        P(),
        P(("expert", "mp"), None),
        P(("expert", "mp"), None),
        P(("expert", "mp"), None),
        P("expert", None, "mp"),
        P("expert", None, "mp"),
        P("expert", "mp", None),
    )

    def body(*args):
        return local(grid, *args)

    return jax.shard_map(
        body, mesh=mesh, in_specs=placed, out_specs=P(("expert", "mp"), None), check_vma=False
    )
```

```python
import functools

import jax
import jax.numpy as jnp
from jax import lax
from jax.experimental import pallas as pl
from jax.experimental.pallas import tpu as pltpu
from jax.sharding import PartitionSpec as P


CAP = 8
META = 128
FFT = 512
OUT = 2048
PLACE = 3072
MIX = 3072
FFN_VMEM = 32 * 2**20
AXES = ("expert", "mp")


class Grid:
    def __init__(self, sizes):
        self.cores = 2
        self.y = sizes["expert"] // self.cores
        self.x = self.y if sizes["mp"] % self.y == 0 else 1
        self.z = sizes["mp"] // self.x

    def index(self, y, c, z, x):
        return ((y * self.cores + c) * self.z + z) * self.x + x

    def move(self, value, to):
        pairs = []
        for y in range(self.y):
            for c in range(self.cores):
                for z in range(self.z):
                    for x in range(self.x):
                        target = to(y, c, z, x)
                        if target is not None:
                            pairs.append((self.index(y, c, z, x), self.index(*target)))
        return lax.ppermute(value, AXES, pairs)

    def first(self, k):
        return lambda y, c, z, x: (
            (y, c, z, (x + k) % self.x) if c == 0 else ((y + k) % self.y, c, z, x)
        )

    def second(self, k):
        return lambda y, c, z, x: (
            ((y + k) % self.y, c, z, x) if c == 0 else (y, c, z, (x + k) % self.x)
        )

    def sibling(self, y, c, z, x):
        return (y, 1 - c, z, x)

    def across_z(self, k, sign=1):
        if self.z & (self.z - 1) == 0:
            return lambda y, c, z, x: (y, c, z ^ k, x)
        return lambda y, c, z, x: (y, c, (z + sign * k) % self.z, x)


def gather_z(grid, own):
    if grid.z != 4:
        return [own] + [grid.move(own, grid.across_z(k)) for k in range(1, grid.z)]
    far = grid.move(own, grid.across_z(2))
    near = grid.move(own, grid.across_z(1))
    last = grid.move(far, grid.across_z(1))
    return [own, near, far, last]


def scatter_z(grid, parts):
    f32 = jnp.float32
    if grid.z != 4:
        moved = [grid.move(parts[k], grid.across_z(k, -1)) for k in range(1, grid.z)]
        return sum([m.astype(f32) for m in moved], parts[0].astype(f32)).astype(jnp.bfloat16)
    own, near, far, last = parts
    last = grid.move(last, grid.across_z(1))
    far = far + last
    far = grid.move(far, grid.across_z(2))
    near = grid.move(near, grid.across_z(1))
    return (own.astype(f32) + far.astype(f32) + near.astype(f32)).astype(jnp.bfloat16)


def spread(grid, block):
    firsts = [block] + [grid.move(block, grid.first(k)) for k in range(1, grid.x)]
    half = jnp.concatenate(firsts, axis=0)
    seconds = [half] + [grid.move(half, grid.second(k)) for k in range(1, grid.y)]
    return jnp.concatenate(seconds, axis=0)


def fold(grid, rows):
    size = rows.shape[0] // grid.y
    moved = [grid.move(rows[k * size : (k + 1) * size], grid.second(-k)) for k in range(1, grid.y)]
    half = sum(moved, rows[:size])
    size = size // grid.x
    moved = [grid.move(half[k * size : (k + 1) * size], grid.first(-k)) for k in range(1, grid.x)]
    return sum(moved, half[:size])


def prepare_kernel(tok_ref, gain_ref, ids_ref, slots_ref, route_ref, out_ref):
    f32, bf16 = jnp.float32, jnp.bfloat16
    _, features = tok_ref.shape
    values = tok_ref[...].astype(f32)
    mean_square = jnp.mean(values * values, axis=1, keepdims=True)
    scale = lax.rsqrt(mean_square + 1e-05)
    for at in range(gain_ref.shape[0]):
        place = slice(at * 128, (at + 1) * 128)
        gain = gain_ref[at : at + 1, :].astype(f32)
        out_ref[:, place] = (values[:, place] * scale * gain).astype(bf16)
    target = (ids_ref[...] * CAP + slots_ref[...]).astype(f32)
    route = route_ref[...]
    shares = route / (route[0:1] + route[1:2])
    high = shares.astype(bf16).astype(f32)
    middle = (shares - high).astype(bf16).astype(f32)
    low = shares - high - middle
    parts = jnp.concatenate([target, high, middle, low], axis=0).astype(bf16)
    row = lax.broadcasted_iota(jnp.int32, (parts.shape[0], META), 0)
    lane = lax.broadcasted_iota(jnp.int32, (parts.shape[0], META), 1)
    select = (row == lane).astype(bf16)
    turned = lax.dot_general(
        parts, select, (((0,), (0,)), ((), ())), preferred_element_type=f32
    )
    out_ref[:, features:] = turned.astype(bf16)


def prepare(tokens, norm_gain, expert_ids, slot_ids, route_weights):
    rows, features = tokens.shape
    return pl.pallas_call(
        prepare_kernel,
        out_shape=jax.ShapeDtypeStruct((rows, features + META), jnp.bfloat16),
        name="prepare",
    )(tokens, norm_gain.reshape(-1, 128), expert_ids.T, slot_ids.T, route_weights.T)


def hits(metas, expert, tok_rows, cores):
    meta = jnp.concatenate(metas, axis=0).astype(jnp.float32)
    count = meta.shape[0]
    each = count // tok_rows * CAP
    block = lax.broadcasted_iota(jnp.int32, (count, 2), 0) // tok_rows * CAP
    places = jnp.full((count, 2), -1.0, jnp.float32)
    for side in range(cores):
        first = ((expert ^ side) * CAP).astype(jnp.float32)
        slots = meta[:, 0:2] - first
        here = (slots >= 0) & (slots < CAP)
        places = jnp.where(here, slots + (block + side * each).astype(jnp.float32), places)
    index = lax.broadcasted_iota(jnp.int32, (count, cores * each), 1).astype(jnp.float32)
    share = meta[:, 2:4] + meta[:, 4:6] + meta[:, 6:8]
    return [index == places[:, k : k + 1] for k in range(2)], share


def place_kernel(n, tok_rows, features, *refs):
    f32, bf16 = jnp.float32, jnp.bfloat16
    blocks, outs = refs[:n], refs[n:]
    expert = lax.axis_index("expert")
    hit, _ = hits([b[:, features:] for b in blocks], expert, tok_rows, len(outs))
    placing = (hit[0] | hit[1]).astype(f32).T.astype(bf16)
    each = outs[0].shape[0]

    @pl.loop(0, features // PLACE)
    def _(j):
        place = pl.ds(pl.multiple_of(j * PLACE, PLACE), PLACE)
        known = jnp.concatenate([b[:, place] for b in blocks], axis=0)
        got = jnp.dot(placing, known, preferred_element_type=f32).astype(bf16)
        for side, out in enumerate(outs):
            out[:, place] = got[side * each : (side + 1) * each]


def place_rows(groups, tok_rows, features):
    count = sum(g.shape[0] for g in groups)
    each = count // tok_rows * CAP
    vmem = pl.BlockSpec(memory_space=pltpu.VMEM)
    out = jax.ShapeDtypeStruct((each, features), jnp.bfloat16)
    return pl.pallas_call(
        functools.partial(place_kernel, len(groups), tok_rows, features),
        out_shape=[out] * 2,
        in_specs=[vmem] * len(groups),
        out_specs=[vmem] * 2,
        cost_estimate=pl.CostEstimate(
            flops=4 * count * each * features, bytes_accessed=4 * count * features, transcendentals=0
        ),
        compiler_params=pltpu.CompilerParams(vmem_limit_bytes=count * 28 * 2**10),
        name="place",
    )(*groups)


def ffn_kernel(features, n, *refs):
    f32, bf16 = jnp.float32, jnp.bfloat16
    blocks, refs = refs[:n], refs[n:]
    gate, up_hbm, down_hbm = refs[:3]
    outs, refs = refs[3:7], refs[7:]
    up, down, gated, hidden, up_sems, down_sems = refs
    width, some = gate.shape[2], outs[0].shape[0]
    up_tiles, down_tiles = width // FFT, features // OUT

    def piece():
        return jnp.concatenate([block[...] for block in blocks], axis=0)

    def tile(i, size):
        return pl.ds(pl.multiple_of(i * size, size), size)

    def up_copy(i):
        place = tile(i, FFT)
        return pltpu.make_async_copy(up_hbm.at[0, :, place], up.at[:, place], up_sems.at[i])

    def down_copy(i):
        place = tile(i, OUT)
        return pltpu.make_async_copy(down_hbm.at[0, :, place], down.at[:, place], down_sems.at[i])

    for i in range(up_tiles):
        up_copy(i).start()

    @pl.loop(0, up_tiles)
    def _(i):
        gate_proj = jnp.dot(piece(), gate[0, :, tile(i, FFT)], preferred_element_type=f32)
        gated[:, tile(i, FFT)] = gate_proj / (1.0 + jnp.exp(-gate_proj))

    for i in range(down_tiles):
        down_copy(i).start()

    @pl.loop(0, up_tiles)
    def _(i):
        up_copy(i).wait()
        up_proj = jnp.dot(piece(), up[:, tile(i, FFT)], preferred_element_type=f32)
        hidden[:, tile(i, FFT)] = (gated[:, tile(i, FFT)] * up_proj).astype(bf16)

    @pl.loop(0, down_tiles)
    def _(i):
        down_copy(i).wait()
        place = tile(i, OUT)
        product = jnp.dot(hidden[...], down[:, place], preferred_element_type=f32)
        product = product.astype(bf16)
        for at, out in enumerate(outs):
            out[:, place] = product[at * some : (at + 1) * some]


def ffn(mine, theirs, w_gate, w_up, w_down):
    bf16 = jnp.bfloat16
    each, features = sum(m.shape[0] for m in mine), mine[0].shape[1]
    width = w_gate.shape[2]
    need = 2 * (3 * features * width + 4 * each * features + 2 * each * width)
    if need > 56 * 2**20 or width % FFT or features % OUT:
        piece = jnp.concatenate(mine + theirs, axis=0)
        gate_proj = jnp.dot(piece, w_gate[0], preferred_element_type=jnp.float32)
        up_proj = jnp.dot(piece, w_up[0], preferred_element_type=jnp.float32)
        hidden = (jax.nn.silu(gate_proj) * up_proj).astype(bf16)
        product = jnp.dot(hidden, w_down[0], preferred_element_type=jnp.float32).astype(bf16)
        return [product[at * each // 2 : (at + 1) * each // 2] for at in range(4)]
    vmem, hbm = pl.BlockSpec(memory_space=pltpu.VMEM), pl.BlockSpec(memory_space=pltpu.HBM)
    return pl.pallas_call(
        functools.partial(ffn_kernel, features, len(mine + theirs)),
        out_shape=[jax.ShapeDtypeStruct((each // 2, features), bf16)] * 4,
        in_specs=[vmem] * (len(mine + theirs) + 1) + [hbm] * 2,
        out_specs=[vmem] * 4,
        scratch_shapes=[
            pltpu.VMEM((features, width), bf16),
            pltpu.VMEM((width, features), bf16),
            pltpu.VMEM((2 * each, width), jnp.float32),
            pltpu.VMEM((2 * each, width), bf16),
            pltpu.SemaphoreType.DMA((width // FFT,)),
            pltpu.SemaphoreType.DMA((features // OUT,)),
        ],
        cost_estimate=pl.CostEstimate(
            flops=12 * each * features * width,
            bytes_accessed=6 * features * width,
            transcendentals=2 * each * width,
        ),
        compiler_params=pltpu.CompilerParams(vmem_limit_bytes=FFN_VMEM),
        name="ffn",
    )(*mine, *theirs, w_gate, w_up, w_down)


def mix_kernel(n, tok_rows, features, *refs):
    f32, bf16 = jnp.float32, jnp.bfloat16
    metas, (mine, theirs), outs = refs[:n], refs[n : n + 2], refs[n + 2 :]
    expert = lax.axis_index("expert")
    hit, share = hits([m[...] for m in metas], expert, tok_rows, 2)
    taking = [h.astype(f32).astype(bf16) for h in hit]

    @pl.loop(0, features // MIX)
    def _(j):
        place = pl.ds(pl.multiple_of(j * MIX, MIX), MIX)
        product = jnp.concatenate([mine[:, place], theirs[:, place]], axis=0)
        total = share[:, 0:1] * jnp.dot(taking[0], product, preferred_element_type=f32)
        total += share[:, 1:2] * jnp.dot(taking[1], product, preferred_element_type=f32)
        total = total.astype(bf16)
        at = 0
        for out in outs:
            out[:, place] = total[at : at + out.shape[0]]
            at += out.shape[0]


def mix(groups, mine, theirs, tok_rows):
    features = mine.shape[1]
    n = len(groups)
    vmem = pl.BlockSpec(memory_space=pltpu.VMEM)
    last = features // META
    metas = [
        pl.BlockSpec((g.shape[0], META), lambda i: (0, last), memory_space=pltpu.VMEM) for g in groups
    ]
    whole = pl.BlockSpec(mine.shape, lambda i: (0, 0))
    count = sum(g.shape[0] for g in groups)
    return pl.pallas_call(
        functools.partial(mix_kernel, n, tok_rows, features),
        grid=(1,),
        out_shape=[jax.ShapeDtypeStruct((g.shape[0], features), jnp.bfloat16) for g in groups],
        in_specs=metas + [whole] * 2,
        out_specs=[pl.BlockSpec((g.shape[0], features), lambda i: (0, 0)) for g in groups],
        cost_estimate=pl.CostEstimate(
            flops=8 * count * mine.shape[0] * features,
            bytes_accessed=4 * count * features,
            transcendentals=0,
        ),
        compiler_params=pltpu.CompilerParams(vmem_limit_bytes=count * 28 * 2**10),
        name="mix",
    )(*groups, mine, theirs)


def local(grid, tokens, norm_gain, expert_ids, slot_ids, route_weights, w_gate, w_up, w_down):
    tok_rows, features = tokens.shape
    own = prepare(tokens, norm_gain, expert_ids, slot_ids, route_weights)
    groups = [spread(grid, block) for block in gather_z(grid, own)]
    mine, theirs = [], []
    for some in (groups[:-1], groups[-1:]):
        kept, away = place_rows(some, tok_rows, features)
        mine.append(kept)
        theirs.append(grid.move(away, grid.sibling))
    results = ffn(mine, theirs, w_gate, w_up, w_down)
    moved = [None, None]
    for side in (1, 0):
        moved[side] = grid.move(results[2 + side], grid.sibling)
    parts = [None] * grid.z
    some = grid.z // 2
    for side in (1, 0):
        held = groups[side * some : (side + 1) * some]
        mixed = mix(held, results[side], moved[side], tok_rows)
        for k in reversed(range(some)):
            parts[side * some + k] = fold(grid, mixed[k])
    return scatter_z(grid, parts)


def solution(mesh):
    grid = Grid(mesh.shape)
    placed = (
        P(("expert", "mp"), None),
        P(),
        P(("expert", "mp"), None),
        P(("expert", "mp"), None),
        P(("expert", "mp"), None),
        P("expert", None, "mp"),
        P("expert", None, "mp"),
        P("expert", "mp", None),
    )

    def body(*args):
        return local(grid, *args)

    return jax.shard_map(
        body, mesh=mesh, in_specs=placed, out_specs=P(("expert", "mp"), None), check_vma=False
    )
```

```python
import functools

import jax
import jax.numpy as jnp
from jax import lax
from jax.experimental import pallas as pl
from jax.experimental.pallas import tpu as pltpu
from jax.sharding import PartitionSpec as P


CAP = 8
META = 128
SPLIT_OUT = (0,)
FFT = 512
OUT = 2048
PLACE = 3072
MIX = 3072
FFN_VMEM = 32 * 2**20
AXES = ("expert", "mp")


class Grid:
    def __init__(self, sizes):
        self.cores = 2
        self.y = sizes["expert"] // self.cores
        self.x = self.y if sizes["mp"] % self.y == 0 else 1
        self.z = sizes["mp"] // self.x

    def index(self, y, c, z, x):
        return ((y * self.cores + c) * self.z + z) * self.x + x

    def move(self, value, to):
        pairs = []
        for y in range(self.y):
            for c in range(self.cores):
                for z in range(self.z):
                    for x in range(self.x):
                        target = to(y, c, z, x)
                        if target is not None:
                            pairs.append((self.index(y, c, z, x), self.index(*target)))
        return lax.ppermute(value, AXES, pairs)

    def first(self, k):
        return lambda y, c, z, x: (
            (y, c, z, (x + k) % self.x) if c == 0 else ((y + k) % self.y, c, z, x)
        )

    def second(self, k):
        return lambda y, c, z, x: (
            ((y + k) % self.y, c, z, x) if c == 0 else (y, c, z, (x + k) % self.x)
        )

    def sibling(self, y, c, z, x):
        return (y, 1 - c, z, x)

    def across_z(self, k, sign=1):
        if self.z & (self.z - 1) == 0:
            return lambda y, c, z, x: (y, c, z ^ k, x)
        return lambda y, c, z, x: (y, c, (z + sign * k) % self.z, x)


def gather_z(grid, own):
    if grid.z != 4:
        return [own] + [grid.move(own, grid.across_z(k)) for k in range(1, grid.z)]
    far = grid.move(own, grid.across_z(2))
    near = grid.move(own, grid.across_z(1))
    return [own, near, far]


def scatter_z(grid, parts):
    f32 = jnp.float32
    if grid.z != 4:
        moved = [grid.move(parts[k], grid.across_z(k, -1)) for k in range(1, grid.z)]
        return sum([m.astype(f32) for m in moved], parts[0].astype(f32)).astype(jnp.bfloat16)
    own, near, far, last = parts
    last = grid.move(last, grid.across_z(1))
    far = far + last
    far = grid.move(far, grid.across_z(2))
    near = grid.move(near, grid.across_z(1))
    return (own.astype(f32) + far.astype(f32) + near.astype(f32)).astype(jnp.bfloat16)


def first_step(grid, block):
    firsts = [block] + [grid.move(block, grid.first(k)) for k in range(1, grid.x)]
    return jnp.concatenate(firsts, axis=0)


def second_step(grid, half):
    seconds = [half] + [grid.move(half, grid.second(k)) for k in range(1, grid.y)]
    return jnp.concatenate(seconds, axis=0)


def fold(grid, rows, at):
    size = rows.shape[0] // grid.y
    one = size // grid.x
    skip = one if at in SPLIT_OUT else 0
    moved = [
        grid.move(rows[k * size + skip : (k + 1) * size], grid.second(-k))
        for k in range(1, grid.y)
    ]
    half = sum(moved, rows[skip:size])
    moved = [
        grid.move(half[k * one - skip : (k + 1) * one - skip], grid.first(-k))
        for k in range(1, grid.x)
    ]
    if at not in SPLIT_OUT:
        return sum(moved, half[:one])
    moved += [grid.move(rows[k * size : k * size + one], grid.second(-k)) for k in range(1, grid.y)]
    return sum([m.astype(jnp.float32) for m in moved], rows[:one].astype(jnp.float32))


def prepare_kernel(tok_ref, gain_ref, ids_ref, slots_ref, route_ref, out_ref):
    f32, bf16 = jnp.float32, jnp.bfloat16
    _, features = tok_ref.shape
    values = tok_ref[...].astype(f32)
    mean_square = jnp.mean(values * values, axis=1, keepdims=True)
    scale = lax.rsqrt(mean_square + 1e-05)
    for at in range(gain_ref.shape[0]):
        place = slice(at * 128, (at + 1) * 128)
        gain = gain_ref[at : at + 1, :].astype(f32)
        out_ref[:, place] = (values[:, place] * scale * gain).astype(bf16)
    target = (ids_ref[...] * CAP + slots_ref[...]).astype(f32)
    route = route_ref[...]
    shares = route / (route[0:1] + route[1:2])
    high = shares.astype(bf16).astype(f32)
    middle = (shares - high).astype(bf16).astype(f32)
    low = shares - high - middle
    parts = jnp.concatenate([target, high, middle, low], axis=0).astype(bf16)
    row = lax.broadcasted_iota(jnp.int32, (parts.shape[0], META), 0)
    lane = lax.broadcasted_iota(jnp.int32, (parts.shape[0], META), 1)
    select = (row == lane).astype(bf16)
    turned = lax.dot_general(
        parts, select, (((0,), (0,)), ((), ())), preferred_element_type=f32
    )
    out_ref[:, features:] = turned.astype(bf16)


def prepare(tokens, norm_gain, expert_ids, slot_ids, route_weights):
    rows, features = tokens.shape
    return pl.pallas_call(
        prepare_kernel,
        out_shape=jax.ShapeDtypeStruct((rows, features + META), jnp.bfloat16),
        name="prepare",
    )(tokens, norm_gain.reshape(-1, 128), expert_ids.T, slot_ids.T, route_weights.T)


def hits(metas, expert, tok_rows, cores):
    meta = jnp.concatenate(metas, axis=0).astype(jnp.float32)
    count = meta.shape[0]
    each = count // tok_rows * CAP
    block = lax.broadcasted_iota(jnp.int32, (count, 2), 0) // tok_rows * CAP
    places = jnp.full((count, 2), -1.0, jnp.float32)
    for side in range(cores):
        first = ((expert ^ side) * CAP).astype(jnp.float32)
        slots = meta[:, 0:2] - first
        here = (slots >= 0) & (slots < CAP)
        places = jnp.where(here, slots + (block + side * each).astype(jnp.float32), places)
    index = lax.broadcasted_iota(jnp.int32, (count, cores * each), 1).astype(jnp.float32)
    share = meta[:, 2:4] + meta[:, 4:6] + meta[:, 6:8]
    return [index == places[:, k : k + 1] for k in range(2)], share


def place_kernel(n, tok_rows, features, *refs):
    f32, bf16 = jnp.float32, jnp.bfloat16
    blocks, outs = refs[:n], refs[n:]
    expert = lax.axis_index("expert")
    hit, _ = hits([b[:, features:] for b in blocks], expert, tok_rows, len(outs))
    placing = (hit[0] | hit[1]).astype(f32).T.astype(bf16)
    each = outs[0].shape[0]

    @pl.loop(0, features // PLACE)
    def _(j):
        place = pl.ds(pl.multiple_of(j * PLACE, PLACE), PLACE)
        known = jnp.concatenate([b[:, place] for b in blocks], axis=0)
        got = jnp.dot(placing, known, preferred_element_type=f32).astype(bf16)
        for side, out in enumerate(outs):
            out[:, place] = got[side * each : (side + 1) * each]


def place_rows(groups, tok_rows, features):
    count = sum(g.shape[0] for g in groups)
    each = count // tok_rows * CAP
    vmem = pl.BlockSpec(memory_space=pltpu.VMEM)
    out = jax.ShapeDtypeStruct((each, features), jnp.bfloat16)
    return pl.pallas_call(
        functools.partial(place_kernel, len(groups), tok_rows, features),
        out_shape=[out] * 2,
        in_specs=[vmem] * len(groups),
        out_specs=[vmem] * 2,
        cost_estimate=pl.CostEstimate(
            flops=4 * count * each * features, bytes_accessed=4 * count * features, transcendentals=0
        ),
        compiler_params=pltpu.CompilerParams(vmem_limit_bytes=count * 28 * 2**10),
        name="place",
    )(*groups)


def ffn_kernel(features, n, *refs):
    f32, bf16 = jnp.float32, jnp.bfloat16
    blocks, refs = refs[:n], refs[n:]
    gate, up_hbm, down_hbm = refs[:3]
    outs, refs = refs[3:7], refs[7:]
    up, down, gated, hidden, up_sems, down_sems = refs
    width = gate.shape[2]
    up_tiles, down_tiles = width // FFT, features // OUT

    def piece():
        return jnp.concatenate([block[...] for block in blocks], axis=0)

    def tile(i, size):
        return pl.ds(pl.multiple_of(i * size, size), size)

    def up_copy(i):
        place = tile(i, FFT)
        return pltpu.make_async_copy(up_hbm.at[0, :, place], up.at[:, place], up_sems.at[i])

    def down_copy(i):
        place = tile(i, OUT)
        return pltpu.make_async_copy(down_hbm.at[0, :, place], down.at[:, place], down_sems.at[i])

    for i in range(up_tiles):
        up_copy(i).start()

    @pl.loop(0, up_tiles)
    def _(i):
        gate_proj = jnp.dot(piece(), gate[0, :, tile(i, FFT)], preferred_element_type=f32)
        gated[:, tile(i, FFT)] = gate_proj / (1.0 + jnp.exp(-gate_proj))

    for i in range(down_tiles):
        down_copy(i).start()

    @pl.loop(0, up_tiles)
    def _(i):
        up_copy(i).wait()
        up_proj = jnp.dot(piece(), up[:, tile(i, FFT)], preferred_element_type=f32)
        hidden[:, tile(i, FFT)] = (gated[:, tile(i, FFT)] * up_proj).astype(bf16)

    @pl.loop(0, down_tiles)
    def _(i):
        down_copy(i).wait()
        place = tile(i, OUT)
        product = jnp.dot(hidden[...], down[:, place], preferred_element_type=f32)
        product = product.astype(bf16)
        at = 0
        for out in outs:
            out[:, place] = product[at : at + out.shape[0]]
            at += out.shape[0]


def fetch_kernel(source, target, sems):
    count = sems.shape[0]
    size = source.shape[1] // count
    copies = [
        pltpu.make_async_copy(
            source.at[:, pl.ds(i * size, size)], target.at[:, pl.ds(i * size, size)], sems.at[i]
        )
        for i in range(count)
    ]
    for copy in copies:
        copy.start()
    for copy in copies:
        copy.wait()


def fetch(weights):
    return pl.pallas_call(
        fetch_kernel,
        out_shape=jax.ShapeDtypeStruct(weights.shape, weights.dtype),
        in_specs=[pl.BlockSpec(memory_space=pltpu.HBM)],
        out_specs=pl.BlockSpec(memory_space=pltpu.VMEM),
        scratch_shapes=[pltpu.SemaphoreType.DMA((8,))],
        cost_estimate=pl.CostEstimate(
            flops=0, bytes_accessed=2 * weights.size * 2, transcendentals=0
        ),
        compiler_params=pltpu.CompilerParams(vmem_limit_bytes=2**20),
        name="fetch",
    )(weights)


def ffn(mine, theirs, w_gate, w_up, w_down):
    bf16 = jnp.bfloat16
    each, features = sum(m.shape[0] for m in mine), mine[0].shape[1]
    lengths = [m.shape[0] for m in mine]
    width = w_gate.shape[2]
    need = 2 * (3 * features * width + 4 * each * features + 2 * each * width)
    if need > 56 * 2**20 or width % FFT or features % OUT:
        piece = jnp.concatenate(mine + theirs, axis=0)
        gate_proj = jnp.dot(piece, w_gate[0], preferred_element_type=jnp.float32)
        up_proj = jnp.dot(piece, w_up[0], preferred_element_type=jnp.float32)
        hidden = (jax.nn.silu(gate_proj) * up_proj).astype(bf16)
        product = jnp.dot(hidden, w_down[0], preferred_element_type=jnp.float32).astype(bf16)
        cuts = [0, lengths[0], each, each + lengths[0], 2 * each]
        return [product[a:b] for a, b in zip(cuts, cuts[1:])]
    w_gate = fetch(w_gate)
    vmem, hbm = pl.BlockSpec(memory_space=pltpu.VMEM), pl.BlockSpec(memory_space=pltpu.HBM)
    return pl.pallas_call(
        functools.partial(ffn_kernel, features, len(mine + theirs)),
        out_shape=[jax.ShapeDtypeStruct((length, features), bf16) for length in 2 * lengths],
        in_specs=[vmem] * (len(mine + theirs) + 1) + [hbm] * 2,
        out_specs=[vmem] * 4,
        scratch_shapes=[
            pltpu.VMEM((features, width), bf16),
            pltpu.VMEM((width, features), bf16),
            pltpu.VMEM((2 * each, width), jnp.float32),
            pltpu.VMEM((2 * each, width), bf16),
            pltpu.SemaphoreType.DMA((width // FFT,)),
            pltpu.SemaphoreType.DMA((features // OUT,)),
        ],
        cost_estimate=pl.CostEstimate(
            flops=12 * each * features * width,
            bytes_accessed=6 * features * width,
            transcendentals=2 * each * width,
        ),
        compiler_params=pltpu.CompilerParams(vmem_limit_bytes=FFN_VMEM),
        name="ffn",
    )(*mine, *theirs, w_gate, w_up, w_down)


def mix_kernel(n, tok_rows, features, *refs):
    f32, bf16 = jnp.float32, jnp.bfloat16
    metas, (mine, theirs), outs = refs[:n], refs[n : n + 2], refs[n + 2 :]
    expert = lax.axis_index("expert")
    hit, share = hits([m[...] for m in metas], expert, tok_rows, 2)
    taking = [h.astype(f32).astype(bf16) for h in hit]

    @pl.loop(0, features // MIX)
    def _(j):
        place = pl.ds(pl.multiple_of(j * MIX, MIX), MIX)
        product = jnp.concatenate([mine[:, place], theirs[:, place]], axis=0)
        total = share[:, 0:1] * jnp.dot(taking[0], product, preferred_element_type=f32)
        total += share[:, 1:2] * jnp.dot(taking[1], product, preferred_element_type=f32)
        total = total.astype(bf16)
        at = 0
        for out in outs:
            out[:, place] = total[at : at + out.shape[0]]
            at += out.shape[0]


def mix(groups, mine, theirs, tok_rows):
    features = mine.shape[1]
    n = len(groups)
    vmem = pl.BlockSpec(memory_space=pltpu.VMEM)
    last = features // META
    metas = [
        pl.BlockSpec((g.shape[0], META), lambda i: (0, last), memory_space=pltpu.VMEM) for g in groups
    ]
    whole = pl.BlockSpec(mine.shape, lambda i: (0, 0))
    count = sum(g.shape[0] for g in groups)
    return pl.pallas_call(
        functools.partial(mix_kernel, n, tok_rows, features),
        grid=(1,),
        out_shape=[jax.ShapeDtypeStruct((g.shape[0], features), jnp.bfloat16) for g in groups],
        in_specs=metas + [whole] * 2,
        out_specs=[pl.BlockSpec((g.shape[0], features), lambda i: (0, 0)) for g in groups],
        cost_estimate=pl.CostEstimate(
            flops=8 * count * mine.shape[0] * features,
            bytes_accessed=4 * count * features,
            transcendentals=0,
        ),
        compiler_params=pltpu.CompilerParams(vmem_limit_bytes=count * 28 * 2**10),
        name="mix",
    )(*groups, mine, theirs)


def local(grid, tokens, norm_gain, expert_ids, slot_ids, route_weights, w_gate, w_up, w_down):
    tok_rows, features = tokens.shape
    own = prepare(tokens, norm_gain, expert_ids, slot_ids, route_weights)
    halves = [first_step(grid, block) for block in gather_z(grid, own)]
    if len(halves) < grid.z:
        halves.append(grid.move(halves[2], grid.across_z(1)))
    groups = [second_step(grid, half) for half in halves]
    mine, theirs = [], []
    for some in (groups[:-1], groups[-1:]):
        kept, away = place_rows(some, tok_rows, features)
        mine.append(kept)
        theirs.append(grid.move(away, grid.sibling))
    results = ffn(mine, theirs, w_gate, w_up, w_down)
    moved = [None, None]
    for side in (1, 0):
        moved[side] = grid.move(results[2 + side], grid.sibling)
    parts = [None] * grid.z
    for side in (1, 0):
        held = list(range(grid.z))[-1:] if side else list(range(grid.z))[:-1]
        mixed = mix([groups[k] for k in held], results[side], moved[side], tok_rows)
        for k in reversed(held):
            parts[k] = fold(grid, mixed[k - held[0]], k)
    return scatter_z(grid, parts)


def solution(mesh):
    grid = Grid(mesh.shape)
    placed = (
        P(("expert", "mp"), None),
        P(),
        P(("expert", "mp"), None),
        P(("expert", "mp"), None),
        P(("expert", "mp"), None),
        P("expert", None, "mp"),
        P("expert", None, "mp"),
        P("expert", "mp", None),
    )

    def body(*args):
        return local(grid, *args)

    return jax.shard_map(
        body, mesh=mesh, in_specs=placed, out_specs=P(("expert", "mp"), None), check_vma=False
    )
```
